32 devices in a mesh: dp: 2 (over y), expert: 16 (over z, x, core).
Axes of the slice: x: 2, y: 2, z: 4, core: 2. Of those that a mesh axis runs over, the one named last changes fastest.
Arguments:
- tokens: bfloat16 [256, 2880], P(('dp', 'expert')), may hold values from -6 to 6
- routes: int32 [2, 256, 4], P(None, ('dp', 'expert')), may hold values from 0 to 15, all different within a row; in each aligned block of 8 rows (0 to 7, 8 to 15, ..., all dimensions but the last counted through in order) at most 4 rows name the same one
- placement: int32 [2, 16], replicated, may hold values from 0 to 15, each once within a row
- up_weight: bfloat16 [2, 16, 2880, 1440], P(None, 'expert', None, 'dp'), may hold values from -0.109375 to 0.109375
- down_weight: bfloat16 [2, 16, 1440, 2880], P(None, 'expert', 'dp'), may hold values from -0.15625 to 0.15625
- router_weight: bfloat16 [2, 16, 2880], P(None, 'expert'), may hold values from -0.21875 to 0.21875
Outputs:
- final_stream: bfloat16 [256, 2880], P(('dp', 'expert'))
The draws below stay inside these ranges and needn't reach their ends.
Inputs may be any that keep to these rules, and one draw needn't show every extreme that they name: `routes`: each row names 4 different experts. Within one layer's rows of one device no expert is named by more than 4 rows, and some device names some expert exactly 4 times. `placement`: each layer's row is a permutation of the slots.
All inputs are finite; a program needn't handle non-finite values.
Results may differ from the reference program's by a relative error of at most 0.008.
Values may be sent and summed in bfloat16 or wider, within the bound.
A program may use at most 64 MiB of HBM per device.

```python
import math
import jax
import jax.numpy as jnp
import numpy as np
from jax import lax

D = 2880
TOPK = 4
FF = 1440
LAYERS = 2
TOK_DEV = 8
EXPERTS = 16
FF_DEV = 720
CAP = 4
TOKENS = 256
N_DP = 2
N_EXPERT = 16


def levels(stream_key, extent, split, least, largest):
    factor_of, own = 1.0, jax.random.fold_in(stream_key, 6)
    for position, parts in split:
        heights = jnp.exp(jax.random.uniform(jax.random.fold_in(own, position), (parts,), jnp.float32, least / len(split), largest / len(split)))
        factor_of = factor_of * jnp.repeat(heights, extent[position] // parts).reshape([-1 if axis == position else 1 for axis in range(len(extent))])
    return factor_of


def assign_block(own_key, own, number, rows, count, top, reach, slope):
    ranking = jax.random.permutation(own_key, count)
    crowded, usual = load_shares(count, rows * top, reach, slope, True), load_shares(count, rows * top, reach, slope, False)
    places = jnp.arange(count)

    def named(sizes, rotation):
        used = int((sizes > 0).sum())
        fixed = max(1, used // 4)
        moved = fixed + (places - fixed + rotation * (used - fixed)) % max(1, count - fixed)
        return jnp.zeros((count,), jnp.int32).at[ranking[jnp.where(places < fixed, places, moved)]].set(jnp.asarray(sizes, jnp.int32))

    sizes = jnp.where(number % 4 == 0, named(crowded, number // 4), named(usual, number - number // 4 - 1))
    mixed = jax.random.permutation(jax.random.fold_in(own, 3), count)
    giver, receiver = mixed[0:count // 2 * 2:2], mixed[1:count // 2 * 2:2]
    room = jnp.minimum(sizes[giver] - 1, reach - sizes[receiver]) // 2
    room = jnp.where((giver == ranking[0]) | (receiver == ranking[0]) | (sizes[receiver] == 0), 0, jnp.maximum(room, 0))
    moved = jax.random.randint(jax.random.fold_in(own, 4), (count // 2,), 0, 1 << 20) % (room + 1)
    sizes = sizes.at[giver].add(-moved).at[receiver].add(moved)
    items = jnp.searchsorted(jnp.cumsum(sizes), jnp.arange(rows * top), side="right").astype(jnp.int32)
    listing = items.reshape(top, rows).T
    listing = listing[jax.random.permutation(jax.random.fold_in(own, 1), rows)]
    rotation = jax.random.randint(jax.random.fold_in(own, 2), (rows, 1), 0, top)
    return jnp.take_along_axis(listing, (jnp.arange(top)[None, :] + rotation) % top, axis=1)


def load_shares(count, total, reach, slope, full):
    portions = [(1 << 20) // math.isqrt(rank ** slope) + 1 for rank in range(1, count + 1)]
    largest = reach if full else min(reach, max(-(-total // count), total * portions[0] // sum(portions)))
    least = 1 if total - largest >= count - 1 else 0
    holding, spare = [largest] + [least] * (count - 1), total - largest - least * (count - 1)
    while spare > 0:
        movable = [i for i in range(1, count) if holding[i] < largest] or [i for i in range(1, count) if holding[i] < reach]
        whole, budget = sum([portions[i] for i in movable]), spare
        for i in movable:
            extra = min(reach - holding[i], max(1, budget * portions[i] // whole), spare)
            holding[i] = holding[i] + extra
            spare = spare - extra
    return np.array(holding)


def bell_draw(key, extent, width, most, split=(), kind=jnp.bfloat16):
    entries = width * jax.random.normal(key, extent, jnp.float32)
    if split:
        entries = entries * levels(key, extent, split, -0.22, 0.18)
    return jnp.clip(entries, -most, most).astype(kind)


def setup_inputs(seed: int = 0) -> dict:
    splits = jax.random.split(jax.random.key(seed), 7)
    tokens = bell_draw(splits[0], (TOKENS, D), 1.0, 6.0, ((0, 32),))
    routes_keys = jax.random.split(jax.random.fold_in(splits[1], 1), LAYERS * TOKENS // TOK_DEV)
    routes_turns = jax.random.permutation(jax.random.fold_in(splits[1], 3), LAYERS * TOKENS // TOK_DEV)
    routes = jax.vmap(lambda own, number: assign_block(jax.random.fold_in(splits[1], 2), own, number, TOK_DEV, EXPERTS, TOPK, CAP, 1))(routes_keys, routes_turns).reshape((LAYERS, TOKENS, TOPK))
    placement = jax.vmap(lambda own: jax.random.permutation(own, EXPERTS))(jax.random.split(splits[2], LAYERS)).reshape((LAYERS, EXPERTS)).astype(jnp.int32)
    up_weight = bell_draw(splits[3], (LAYERS, EXPERTS, D, FF), D ** -0.5, 0.109375, ((1, 16), (3, 2)))
    down_weight = bell_draw(splits[4], (LAYERS, EXPERTS, FF, D), FF ** -0.5, 0.15625, ((1, 16), (2, 2)))
    router_weight = bell_draw(splits[5], (LAYERS, EXPERTS, D), (D // 4) ** -0.5, 0.21875, ((1, 16),))
    return dict(tokens=tokens, routes=routes, placement=placement, up_weight=up_weight, down_weight=down_weight, router_weight=router_weight)


def rms_rows(stream):
    values = stream.astype(jnp.float32)
    inverse = lax.rsqrt(lax.optimization_barrier(jnp.mean(values * values, axis=-1, keepdims=True)) + 1e-05)
    return (values * inverse).astype(jnp.bfloat16)

def layer_step(stream, packed):
    route_rows, place_row, up_layer, down_layer, router_layer = packed
    normed = rms_rows(stream)
    target = place_row[route_rows].reshape(-1).astype(jnp.int32)
    row_order = jnp.argsort(target, stable=True).astype(jnp.int32)
    sorted_target = target[row_order]
    slot_ids = jnp.arange(EXPERTS, dtype=jnp.int32)
    counts = lax.optimization_barrier(jnp.sum((target[:, None] == slot_ids[None, :]).astype(jnp.int32), axis=0))
    starts = (jnp.cumsum(counts) - counts).astype(jnp.int32)
    slot_rows = N_DP * N_EXPERT * CAP
    picked = jnp.concatenate([normed[row_order // TOPK], jnp.zeros((slot_rows, D), jnp.bfloat16)], axis=0)

    def per_slot(slot_index):
        slot_in = lax.dynamic_slice_in_dim(picked, starts[slot_index], slot_rows, 0)
        hidden = jax.nn.silu(jnp.dot(slot_in, up_layer[slot_index], preferred_element_type=jnp.float32)).astype(jnp.bfloat16)
        blocks = hidden.astype(jnp.float32).reshape(slot_rows, N_DP, FF_DEV)
        down_blocks = down_layer[slot_index].astype(jnp.float32).reshape(N_DP, FF_DEV, D)
        part_sums = jnp.einsum('rbf,bfd->rbd', blocks, down_blocks).astype(jnp.bfloat16)
        output = lax.optimization_barrier(jnp.sum(part_sums.astype(jnp.float32), axis=1))
        affinity = jax.nn.sigmoid(jnp.dot(slot_in, router_layer[slot_index], preferred_element_type=jnp.float32)).astype(jnp.bfloat16)
        return (output, affinity)
    outputs, affinity = lax.map(per_slot, slot_ids)
    within = jnp.arange(target.shape[0], dtype=jnp.int32) - starts[sorted_target]
    sorted_out = outputs[sorted_target, within]
    sorted_gate = affinity[sorted_target, within]
    row_out = jnp.zeros_like(sorted_out).at[row_order].set(sorted_out).reshape(-1, TOPK, D)
    row_gate = jnp.zeros_like(sorted_gate).at[row_order].set(sorted_gate).reshape(-1, TOPK).astype(jnp.float32)
    numerator = lax.optimization_barrier(jnp.sum(row_gate[:, :, None] * row_out, axis=1))
    denominator = jnp.maximum(lax.optimization_barrier(jnp.sum(row_gate, axis=1)), 0.5)
    updated = stream.astype(jnp.float32) + numerator / denominator[:, None]
    return (updated.astype(jnp.bfloat16), None)

def reference(tokens, routes, placement, up_weight, down_weight, router_weight):
    result_stream, unused = lax.scan(layer_step, tokens, (routes, placement, up_weight, down_weight, router_weight))
    return result_stream
```

```python
import functools

import jax
import jax.numpy as jnp
from jax import lax
from jax.experimental import pallas as pl
from jax.experimental.pallas import tpu as pltpu
from jax.sharding import PartitionSpec as P


def rms_rows(stream):
    values = stream.astype(jnp.float32)
    inverse = lax.rsqrt(jnp.mean(values * values, axis=-1, keepdims=True) + 1e-05)
    return (values * inverse).astype(jnp.bfloat16)


def slot_table(route_rows, place_row, columns, capacity):
    tok_rows, top_k = route_rows.shape
    experts = place_row.shape[0]
    matches = route_rows[:, :, None] == jnp.arange(experts, dtype=jnp.int32)[None, None, :]
    target = jnp.sum(jnp.where(matches, place_row[None, None, :], 0), axis=2).reshape(-1)
    row_count = target.shape[0]
    positions = jnp.arange(row_count, dtype=jnp.int32)
    earlier = (positions[None, :] < positions[:, None]) & (target[None, :] == target[:, None])
    row_rank = jnp.sum(earlier.astype(jnp.int32), axis=1)
    placed = (target[:, None, None] == jnp.arange(columns, dtype=jnp.int32)[None, :, None]) & (
        row_rank[:, None, None] == jnp.arange(capacity, dtype=jnp.int32)[None, None, :]
    )
    slot_map = jnp.sum(
        placed.reshape(tok_rows, top_k, columns, capacity).astype(jnp.float32), axis=1
    )
    return jnp.transpose(slot_map, (1, 2, 0))


def plan_by_collectives(tokens, routes, placement, up_weight, down_weight, router_weight):
    groups = lax.axis_size("dp")
    columns = lax.axis_size("expert")
    tok_rows = tokens.shape[0]
    top_k = routes.shape[2]
    capacity = 2 * tok_rows * top_k // columns

    def layer_step(stream, packed):
        route_rows, place_row, up_part, down_part, router_part = packed
        normed = rms_rows(stream)
        slot_map = slot_table(route_rows, place_row, columns, capacity)
        outgoing = jnp.einsum(
            "jct,td->jcd", slot_map.astype(jnp.bfloat16), normed, preferred_element_type=jnp.float32
        ).astype(jnp.bfloat16)
        arrived = lax.all_to_all(
            outgoing, "expert", split_axis=0, concat_axis=0, tiled=True
        ).reshape(columns * capacity, -1)
        affinity = jax.nn.sigmoid(
            jnp.dot(arrived, router_part[0], preferred_element_type=jnp.float32)
        ).astype(jnp.bfloat16)
        all_rows, all_gates = (
            lax.all_gather(arrived, "dp", axis=0, tiled=True),
            lax.all_gather(affinity, "dp", axis=0, tiled=True),
        )
        hidden = jax.nn.silu(
            jnp.dot(all_rows, up_part[0], preferred_element_type=jnp.float32)
        ).astype(jnp.bfloat16)
        part_sums = jnp.dot(hidden, down_part[0], preferred_element_type=jnp.float32).astype(
            jnp.bfloat16
        )
        part_sums = part_sums.reshape(groups, columns, capacity, -1)
        all_gates = all_gates.reshape(groups, columns, capacity)
        returned, gates_back = (
            lax.all_to_all(
                lax.all_to_all(part_sums, "dp", split_axis=0, concat_axis=0, tiled=True),
                "expert",
                split_axis=1,
                concat_axis=1,
                tiled=True,
            ),
            lax.all_to_all(
                lax.all_to_all(all_gates, "dp", split_axis=0, concat_axis=0, tiled=True),
                "expert",
                split_axis=1,
                concat_axis=1,
                tiled=True,
            ),
        )
        weights = slot_map * gates_back[0].astype(jnp.float32)[:, :, None]
        numerator = jnp.einsum(
            "ect,gecd->td",
            weights.astype(jnp.bfloat16),
            returned,
            preferred_element_type=jnp.float32,
        )
        denominator = jnp.sum(weights, axis=(0, 1))
        updated = stream.astype(jnp.float32) + numerator / jnp.maximum(denominator, 0.5)[:, None]
        return (updated.astype(jnp.bfloat16), None)

    result_stream, unused = lax.scan(
        layer_step, tokens, (routes, placement, up_weight, down_weight, router_weight)
    )
    return result_stream


LANES = 128
PARTS = 4
MESH = pl.DeviceIdType.MESH


def fused_layers(
    dims, init_ref, aux_ref, up_hbm, down_hbm, down_tail, out_ref,
    pair, masks, stream, wide, shares, rows_in, up_v, down_v, acc, kept,
    core_out, core_in, sums, in_a, mid, in_b, last, in_z, full,
    w_sem, first_send, first_recv, send_sem, recv_sem,
):
    layers, depth, ny, nz, width, tok = dims
    cols = width // (2 * PARTS)
    main = depth // LANES * LANES
    half_rows = 2 * tok
    count = ny * nz * 2 * half_rows
    whole_chunks = main // cols
    y, e = lax.axis_index("dp"), lax.axis_index("expert")
    core, x, z = e % 2, (e // 2) % 2, e // 4
    home = core * PARTS
    away = (1 - core) * PARTS

    def device(y_to, z_to, x_to, core_to):
        return (y_to, (z_to * 2 + x_to) * 2 + core_to)

    weight_copies = []
    for l in range(layers):
        copies = [pltpu.make_async_copy(up_hbm.at[l, 0], up_v.at[l, pl.ds(0, depth)], w_sem.at[l, 0])]
        for k in range(whole_chunks):
            copies.append(pltpu.make_async_copy(
                down_hbm.at[l, 0, :, pl.ds(k * cols, cols)], down_v.at[l, k], w_sem.at[l, 1 + k]))
        rest = main - whole_chunks * cols
        if rest:
            copies.append(pltpu.make_async_copy(
                down_hbm.at[l, 0, :, pl.ds(whole_chunks * cols, rest)],
                down_v.at[l, whole_chunks, :, pl.ds(0, rest)], w_sem.at[l, 1 + whole_chunks]))
        copies.append(pltpu.make_async_copy(
            down_tail.at[l], down_v.at[l, whole_chunks, :, pl.ds(rest, width - main)], w_sem.at[l, 2 + whole_chunks]))
        for copy in copies:
            copy.start()
        weight_copies.append(copies)

    peers = [device(y, z, x, 1 - core), device(y, z, 1 - x, core)]
    peers += [device((y + o) % ny, z, x, core) for o in range(1, ny)]
    peers += [device(y, (z + o) % nz, x, core) for o in range(1, nz)]
    barrier = pltpu.get_barrier_semaphore()
    for peer in peers:
        pl.semaphore_signal(barrier, inc=1, device_id=peer, device_id_type=MESH)
    pl.semaphore_wait(barrier, len(peers))

    first = pltpu.make_async_remote_copy(
        src_ref=init_ref, dst_ref=pair, send_sem=first_send, recv_sem=first_recv,
        device_id=device(y, z, x, 1 - core), device_id_type=MESH)
    first.start()
    for l in range(layers):
        up_v[l, depth:width, :] = jnp.zeros((width - depth, up_v.shape[2]), jnp.bfloat16)
    first.wait()
    mine, other = init_ref[...].astype(jnp.float32), pair[...].astype(jnp.float32)
    both = jnp.concatenate(
        [jnp.where(core == 0, mine, other), jnp.where(core == 0, other, mine)], axis=0)
    stream[...] = both[:, :width]
    for l in range(layers):
        start = width + l * (width - main)
        masks[l] = both[:, start:start + width - main]

    lane = lax.broadcasted_iota(jnp.int32, (half_rows, width), 1)
    for l in range(layers):
        pending = []
        slot = [0]

        def send(src, dst, peer):
            n = slot[0]
            slot[0] = n + 1
            copy = pltpu.make_async_remote_copy(
                src_ref=src, dst_ref=dst, send_sem=send_sem.at[l, n], recv_sem=recv_sem.at[l, n],
                device_id=peer, device_id_type=MESH)
            copy.start()
            pending.append(copy)
            return copy

        def arrived(copies):
            for copy in copies:
                copy.wait_recv()

        values = stream[...]
        inverse = lax.rsqrt(jnp.sum(values * values, axis=-1, keepdims=True) / depth + 1e-05)
        wide[...] = values * inverse
        wide[:, main:width] += masks[l]
        for k in range(2 * PARTS):
            shares[l, k] = wide[:, k * cols:(k + 1) * cols].astype(jnp.bfloat16)

        step = []
        for j in range(PARTS):
            k = home + j
            step.append([
                send(shares.at[l, k], rows_in.at[l, k, y, z, x], device(y, (z + o) % nz, x, core))
                for o in range(1, nz)])
        for j in range(PARTS):
            rows_in[l, home + j, y, z, x] = shares[l, home + j]
        next_step = []
        for j in range(PARTS):
            k = home + j
            arrived(step[j])
            if j % 2 == 0:
                next_step.append([send(rows_in.at[l, k, y, :, x], rows_in.at[l, k, y, :, x], device(y, z, 1 - x, core))])
            else:
                next_step.append([
                    send(rows_in.at[l, k, y, :, x], rows_in.at[l, k, y, :, x], device((y + o) % ny, z, x, core))
                    for o in range(1, ny)])
        step, next_step = next_step, []
        for j in range(PARTS):
            k = home + j
            arrived(step[j])
            if j % 2 == 0:
                next_step.append([
                    send(rows_in.at[l, k, y], rows_in.at[l, k, y], device((y + o) % ny, z, x, core))
                    for o in range(1, ny)])
            else:
                next_step.append([send(rows_in.at[l, k, :, :, x], rows_in.at[l, k, :, :, x], device(y, z, 1 - x, core))])
        step, next_step = next_step, []
        weight_copies[l][0].wait()

        def multiply(k, opening):
            block = rows_in[l, k].reshape(count, cols)
            grown = jnp.dot(block, up_v[l, pl.ds(pl.multiple_of(k * cols, cols), cols), :], preferred_element_type=jnp.float32)
            gates = lax.dot_general(block, aux_ref[l, k], (((1,), (1,)), ((), ())), preferred_element_type=jnp.float32)
            if opening:
                acc[...] = grown
                kept[...] = gates
            else:
                acc[...] += grown
                kept[...] += gates

        for j in range(PARTS):
            arrived(step[j])
            next_step.append([send(rows_in.at[l, home + j], rows_in.at[l, home + j], device(y, z, x, 1 - core))])
            multiply(home + j, j == 0)
        step = next_step
        for j in range(PARTS):
            arrived(step[j])
            multiply(away + j, False)

        before = acc[...]
        hidden = (before / (1.0 + jnp.exp(-before))).astype(jnp.bfloat16)
        affinity = jax.nn.sigmoid(kept[:, 0:1]).astype(jnp.bfloat16).astype(jnp.float32)
        gate = affinity * kept[:, 1:2]
        counts_once = jnp.where(y == 0, 1.0, 0.0)
        for copy in weight_copies[l][1:]:
            copy.wait()

        def outcome(k):
            part = jnp.dot(hidden, down_v[l, k], preferred_element_type=jnp.float32)
            marker = aux_ref[l, k].astype(jnp.float32)[1:2] * counts_once
            return gate * (part + marker)

        step, next_step = [], []
        for j in range(PARTS):
            core_out[l, j] = outcome(away + j).astype(jnp.bfloat16)
            step.append([send(core_out.at[l, j], core_in.at[l, j], device(y, z, x, 1 - core))])
        for j in range(PARTS):
            own = outcome(home + j)
            arrived(step[j])
            total = (own + core_in[l, j].astype(jnp.float32)).astype(jnp.bfloat16)
            sums[l, j] = total.reshape(ny, nz, 2, half_rows, cols)
            if j % 2 == 0:
                next_step.append([
                    send(sums.at[l, j, (y + o) % ny], in_a[0].at[l, j // 2, o - 1], device((y + o) % ny, z, x, core))
                    for o in range(1, ny)])
            else:
                next_step.append([send(sums.at[l, j, :, :, 1 - x], in_a[1].at[l, j // 2], device(y, z, 1 - x, core))])
        step, next_step = next_step, []
        for j in range(PARTS):
            arrived(step[j])
            i = j // 2
            if j % 2 == 0:
                total = sums[l, j, y].astype(jnp.float32)
                for o in range(1, ny):
                    total += in_a[0][l, i, o - 1].astype(jnp.float32)
                mid[0][l, i] = total.astype(jnp.bfloat16)
                next_step.append([send(mid[0].at[l, i, :, 1 - x], in_b.at[l, j, 0], device(y, z, 1 - x, core))])
            else:
                total = sums[l, j, :, :, x].astype(jnp.float32) + in_a[1][l, i].astype(jnp.float32)
                mid[1][l, i] = total.astype(jnp.bfloat16)
                next_step.append([
                    send(mid[1].at[l, i, (y + o) % ny], in_b.at[l, j, o - 1], device((y + o) % ny, z, x, core))
                    for o in range(1, ny)])
        step, next_step = next_step, []
        for j in range(PARTS):
            arrived(step[j])
            i = j // 2
            if j % 2 == 0:
                total = mid[0][l, i, :, x].astype(jnp.float32) + in_b[l, j, 0].astype(jnp.float32)
            else:
                total = mid[1][l, i, y].astype(jnp.float32)
                for o in range(1, ny):
                    total += in_b[l, j, o - 1].astype(jnp.float32)
            last[l, j] = total.astype(jnp.bfloat16)
            next_step.append([
                send(last.at[l, j, (z + o) % nz], in_z.at[l, j, o - 1], device(y, (z + o) % nz, x, core))
                for o in range(1, nz)])
        step = next_step
        for j in range(PARTS):
            arrived(step[j])
            total = last[l, j, z].astype(jnp.float32)
            for o in range(1, nz):
                total += in_z[l, j, o - 1].astype(jnp.float32)
            full[l, home + j] = total.astype(jnp.bfloat16)
        arrived([send(full.at[l, pl.ds(home, PARTS)], full.at[l, pl.ds(home, PARTS)], device(y, z, x, 1 - core))])
        for k in range(2 * PARTS):
            wide[:, k * cols:(k + 1) * cols] = full[l, k].astype(jnp.float32)
        raw = wide[...]
        denominator = jnp.sum(jnp.where(lane < depth, 0.0, raw), axis=-1, keepdims=True)
        updated = stream[...] + jnp.where(lane < depth, raw, 0.0) / jnp.maximum(denominator, 0.5)
        stream[...] = updated.astype(jnp.bfloat16).astype(jnp.float32)
        for copy in pending:
            copy.wait_send()
    result = jnp.where(core == 0, stream[0:tok, :depth], stream[tok:half_rows, :depth])
    out_ref[...] = result.astype(jnp.bfloat16)


def plan_by_kernel(tokens, routes, placement, up_weight, down_weight, router_weight):
    ny, columns = lax.axis_size("dp"), lax.axis_size("expert")
    nz = columns // 4
    tok, depth = tokens.shape
    layers, experts = placement.shape
    block = up_weight.shape[3]
    width = padded_width(depth, experts)
    cols = width // (2 * PARTS)
    main = depth // LANES * LANES
    half_rows = 2 * tok
    count = ny * columns * tok
    slots = jnp.arange(experts, dtype=jnp.int32)
    place_of = jnp.sum(
        jnp.where(routes[..., None] == slots, placement[:, None, None, :], 0), axis=3)
    routed = jnp.any(place_of[..., None] == slots, axis=2).astype(jnp.bfloat16)
    marks = jnp.pad(routed, ((0, 0), (0, 0), (depth - main, width - depth - experts)))
    init = jnp.concatenate(
        [jnp.pad(tokens, ((0, 0), (0, width - depth)))] + [marks[l] for l in range(layers)], axis=1)
    router_row = jnp.pad(router_weight[:, 0], ((0, 0), (0, width - depth)))
    own = (jnp.arange(width, dtype=jnp.int32) == depth + lax.axis_index("expert")).astype(jnp.bfloat16)
    aux = jnp.stack([router_row, jnp.broadcast_to(own, router_row.shape)], axis=1)
    aux = jnp.pad(aux, ((0, 0), (0, 14), (0, 0)))
    aux = jnp.transpose(aux.reshape(layers, 16, 2 * PARTS, cols), (0, 2, 1, 3))
    down_tail = jnp.pad(down_weight[:, 0, :, main:], ((0, 0), (0, 0), (0, width - depth)))
    sends = PARTS * (2 * (nz - 1) + 2 * ny + 2) + 1
    bf16, f32 = jnp.bfloat16, jnp.float32
    in_vmem, anywhere = pl.BlockSpec(memory_space=pltpu.VMEM), pl.BlockSpec(memory_space=pl.ANY)
    return pl.pallas_call(
        functools.partial(fused_layers, (layers, depth, ny, nz, width, tok)),
        out_shape=jax.ShapeDtypeStruct((tok, depth), bf16),
        in_specs=[in_vmem, in_vmem, anywhere, anywhere, anywhere],
        out_specs=in_vmem,
        scratch_shapes=[
            pltpu.VMEM(init.shape, bf16),
            pltpu.VMEM((layers, half_rows, width - main), f32),
            pltpu.VMEM((half_rows, width), f32),
            pltpu.VMEM((half_rows, width), f32),
            pltpu.VMEM((layers, 2 * PARTS, half_rows, cols), bf16),
            pltpu.VMEM((layers, 2 * PARTS, ny, nz, 2, half_rows, cols), bf16),
            pltpu.VMEM((layers, width, block), bf16),
            pltpu.VMEM((layers, 2 * PARTS, block, cols), bf16),
            pltpu.VMEM((count, block), f32),
            pltpu.VMEM((count, 16), f32),
            pltpu.VMEM((layers, PARTS, count, cols), bf16),
            pltpu.VMEM((layers, PARTS, count, cols), bf16),
            pltpu.VMEM((layers, PARTS, ny, nz, 2, half_rows, cols), bf16),
            [
                pltpu.VMEM((layers, PARTS // 2, ny - 1, nz, 2, half_rows, cols), bf16),
                pltpu.VMEM((layers, PARTS // 2, ny, nz, half_rows, cols), bf16),
            ],
            [
                pltpu.VMEM((layers, PARTS // 2, nz, 2, half_rows, cols), bf16),
                pltpu.VMEM((layers, PARTS // 2, ny, nz, half_rows, cols), bf16),
            ],
            pltpu.VMEM((layers, PARTS, ny - 1, nz, half_rows, cols), bf16),
            pltpu.VMEM((layers, PARTS, nz, half_rows, cols), bf16),
            pltpu.VMEM((layers, PARTS, nz - 1, half_rows, cols), bf16),
            pltpu.VMEM((layers, 2 * PARTS, half_rows, cols), bf16),
            pltpu.SemaphoreType.DMA((layers, 3 + main // cols)),
            pltpu.SemaphoreType.DMA,
            pltpu.SemaphoreType.DMA,
            pltpu.SemaphoreType.DMA((layers, sends)),
            pltpu.SemaphoreType.DMA((layers, sends)),
        ],
        compiler_params=pltpu.CompilerParams(
            collective_id=0, has_side_effects=True, vmem_limit_bytes=VMEM_BYTES),
    )(init, aux, up_weight, down_weight, down_tail)


VMEM_BYTES = 60 << 20


def padded_width(depth, experts):
    unit = 2 * PARTS * LANES
    return -(-(depth + experts) // unit) * unit


def kernel_fits(ny, columns, tokens, placement, up_weight):
    tok, depth = tokens.shape
    layers, experts = placement.shape
    block = up_weight.shape[3]
    width = padded_width(depth, experts)
    main = depth // LANES * LANES
    count = ny * columns * tok
    lanes = -(-block // LANES) * LANES
    need = layers * 2 * width * (2 * lanes + 4 * count) + 4 * count * (3 * lanes + width // 4)
    return (
        ny > 1 and columns % 4 == 0 and columns > 4 and experts == columns and up_weight.shape[1] == 1
        and tok % 8 == 0 and depth % 16 == 0 and block % 16 == 0
        and width - main <= width // (2 * PARTS) and need < VMEM_BYTES
    )


def per_device(tokens, routes, placement, up_weight, down_weight, router_weight):
    fits = kernel_fits(lax.axis_size("dp"), lax.axis_size("expert"), tokens, placement, up_weight)
    plan = plan_by_kernel if fits else plan_by_collectives
    return plan(tokens, routes, placement, up_weight, down_weight, router_weight)


def solution(mesh):
    return jax.shard_map(
        per_device,
        mesh=mesh,
        in_specs=(
            P(("dp", "expert"), None),
            P(None, ("dp", "expert"), None),
            P(),
            P(None, "expert", None, "dp"),
            P(None, "expert", "dp", None),
            P(None, "expert", None),
        ),
        out_specs=P(("dp", "expert"), None),
        check_vma=False,
    )
```

```python
import functools

import jax
import jax.numpy as jnp
from jax import lax
from jax.experimental import pallas as pl
from jax.experimental.pallas import tpu as pltpu
from jax.sharding import PartitionSpec as P


def rms_rows(stream):
    values = stream.astype(jnp.float32)
    inverse = lax.rsqrt(jnp.mean(values * values, axis=-1, keepdims=True) + 1e-05)
    return (values * inverse).astype(jnp.bfloat16)


def slot_table(route_rows, place_row, columns, capacity):
    tok_rows, top_k = route_rows.shape
    experts = place_row.shape[0]
    matches = route_rows[:, :, None] == jnp.arange(experts, dtype=jnp.int32)[None, None, :]
    target = jnp.sum(jnp.where(matches, place_row[None, None, :], 0), axis=2).reshape(-1)
    row_count = target.shape[0]
    positions = jnp.arange(row_count, dtype=jnp.int32)
    earlier = (positions[None, :] < positions[:, None]) & (target[None, :] == target[:, None])
    row_rank = jnp.sum(earlier.astype(jnp.int32), axis=1)
    placed = (target[:, None, None] == jnp.arange(columns, dtype=jnp.int32)[None, :, None]) & (
        row_rank[:, None, None] == jnp.arange(capacity, dtype=jnp.int32)[None, None, :]
    )
    slot_map = jnp.sum(
        placed.reshape(tok_rows, top_k, columns, capacity).astype(jnp.float32), axis=1
    )
    return jnp.transpose(slot_map, (1, 2, 0))


def plan_by_collectives(tokens, routes, placement, up_weight, down_weight, router_weight):
    groups = lax.axis_size("dp")
    columns = lax.axis_size("expert")
    tok_rows = tokens.shape[0]
    top_k = routes.shape[2]
    capacity = 2 * tok_rows * top_k // columns

    def layer_step(stream, packed):
        route_rows, place_row, up_part, down_part, router_part = packed
        normed = rms_rows(stream)
        slot_map = slot_table(route_rows, place_row, columns, capacity)
        outgoing = jnp.einsum(
            "jct,td->jcd", slot_map.astype(jnp.bfloat16), normed, preferred_element_type=jnp.float32
        ).astype(jnp.bfloat16)
        arrived = lax.all_to_all(
            outgoing, "expert", split_axis=0, concat_axis=0, tiled=True
        ).reshape(columns * capacity, -1)
        affinity = jax.nn.sigmoid(
            jnp.dot(arrived, router_part[0], preferred_element_type=jnp.float32)
        ).astype(jnp.bfloat16)
        all_rows, all_gates = (
            lax.all_gather(arrived, "dp", axis=0, tiled=True),
            lax.all_gather(affinity, "dp", axis=0, tiled=True),
        )
        hidden = jax.nn.silu(
            jnp.dot(all_rows, up_part[0], preferred_element_type=jnp.float32)
        ).astype(jnp.bfloat16)
        part_sums = jnp.dot(hidden, down_part[0], preferred_element_type=jnp.float32).astype(
            jnp.bfloat16
        )
        part_sums = part_sums.reshape(groups, columns, capacity, -1)
        all_gates = all_gates.reshape(groups, columns, capacity)
        returned, gates_back = (
            lax.all_to_all(
                lax.all_to_all(part_sums, "dp", split_axis=0, concat_axis=0, tiled=True),
                "expert",
                split_axis=1,
                concat_axis=1,
                tiled=True,
            ),
            lax.all_to_all(
                lax.all_to_all(all_gates, "dp", split_axis=0, concat_axis=0, tiled=True),
                "expert",
                split_axis=1,
                concat_axis=1,
                tiled=True,
            ),
        )
        weights = slot_map * gates_back[0].astype(jnp.float32)[:, :, None]
        numerator = jnp.einsum(
            "ect,gecd->td",
            weights.astype(jnp.bfloat16),
            returned,
            preferred_element_type=jnp.float32,
        )
        denominator = jnp.sum(weights, axis=(0, 1))
        updated = stream.astype(jnp.float32) + numerator / jnp.maximum(denominator, 0.5)[:, None]
        return (updated.astype(jnp.bfloat16), None)

    result_stream, unused = lax.scan(
        layer_step, tokens, (routes, placement, up_weight, down_weight, router_weight)
    )
    return result_stream


LANES = 128
PARTS = 4
ORDERS = ("zxy", "zyx", "xzy", "yzx")
SECOND, THIRD = (2, 3, 0, 1), (0, 1, 2, 3)
MESH = pl.DeviceIdType.MESH


def fused_layers(
    dims, tokens_ref, routes_ref, placement_ref, router_ref, up_hbm, down_hbm, out_ref,
    marks, pair, pair_marks, aux_ref, tail_up, tail_down, masks, stream, wide, shares, rows_in, up_v, down_v, acc, kept,
    core_out, core_in, sums, in_a, mid, in_b, last, in_z, full,
    w_sem, first_send, first_recv, send_sem, recv_sem,
):
    layers, depth, ny, nz, width, tok, top_k, experts = dims
    cols = width // (2 * PARTS)
    main = depth // LANES * LANES
    half_rows = 2 * tok
    count = ny * nz * 2 * half_rows
    edge = (2 * PARTS - 1) * cols
    y, e = lax.axis_index("dp"), lax.axis_index("expert")
    core, x, z = e % 2, (e // 2) % 2, e // 4
    home = core * PARTS

    def device(y_to, z_to, x_to, core_to):
        return (y_to, (z_to * 2 + x_to) * 2 + core_to)

    weight_copies = []
    for l in range(layers):
        copies = [
            pltpu.make_async_copy(up_hbm.at[l, 0], up_v.at[l], w_sem.at[l, 0]),
            pltpu.make_async_copy(down_hbm.at[l, 0], down_v.at[l], w_sem.at[l, 1]),
        ]
        for copy in copies:
            copy.start()
        weight_copies.append(copies)

    peers = [device(y, z, x, 1 - core), device(y, z, 1 - x, core)]
    peers += [device((y + o) % ny, z, x, core) for o in range(1, ny)]
    peers += [device(y, (z + o) % nz, x, core) for o in range(1, nz)]
    barrier = pltpu.get_barrier_semaphore()
    for peer in peers:
        pl.semaphore_signal(barrier, inc=1, device_id=peer, device_id_type=MESH)
    pl.semaphore_wait(barrier, len(peers))

    partner = device(y, z, x, 1 - core)
    first = pltpu.make_async_remote_copy(
        src_ref=tokens_ref, dst_ref=pair, send_sem=first_send.at[0], recv_sem=first_recv.at[0],
        device_id=partner, device_id_type=MESH)
    first.start()
    expert_row = lax.broadcasted_iota(jnp.int32, (tok, experts), 1)
    slot_row = lax.broadcasted_iota(jnp.int32, (width - main, experts), 0) - (depth - main)
    for l in range(layers):
        hits = jnp.zeros((tok, experts), jnp.float32)
        for k in range(top_k):
            hits += jnp.where(routes_ref[l, :, k:k + 1] == expert_row, 1.0, 0.0)
        served = jnp.where(placement_ref[l:l + 1, :] == slot_row, 1.0, 0.0)
        marks[l] = lax.dot_general(
            hits.astype(jnp.bfloat16), served.astype(jnp.bfloat16), (((1,), (1,)), ((), ())),
            preferred_element_type=jnp.float32).astype(jnp.bfloat16)
    second = pltpu.make_async_remote_copy(
        src_ref=marks, dst_ref=pair_marks, send_sem=first_send.at[1], recv_sem=first_recv.at[1],
        device_id=partner, device_id_type=MESH)
    second.start()
    lane = lax.broadcasted_iota(jnp.int32, (half_rows, width), 1)
    row = lax.broadcasted_iota(jnp.int32, (half_rows, width), 0)
    for l in range(layers):
        wide[...] = jnp.where((row == 1) & (lane == depth + e), 1.0, 0.0)
        wide[0:1, 0:depth] = router_ref[l:l + 1, :].astype(jnp.float32)
        for k in range(2 * PARTS):
            aux_ref[l, k] = wide[:, k * cols:(k + 1) * cols].astype(jnp.bfloat16)
    stream[...] = jnp.zeros_like(stream)

    def paired(mine, other):
        mine, other = mine.astype(jnp.float32), other.astype(jnp.float32)
        return jnp.concatenate(
            [jnp.where(core == 0, mine, other), jnp.where(core == 0, other, mine)], axis=0)

    first.wait()
    stream[:, 0:depth] = paired(tokens_ref[...], pair[...])
    second.wait()
    for l in range(layers):
        masks[l] = paired(marks[l], pair_marks[l])

    def fill_tail(tail, whole, l):
        tail[l] = jnp.zeros(tail.shape[1:], jnp.bfloat16)
        tail[l, :, 0:depth - edge] = whole[l, :, edge:depth]

    def chunk(whole, tail, l, side, j):
        if j < PARTS - 1:
            return whole[l, :, pl.ds(pl.multiple_of((side * PARTS + j) * cols, cols), cols)]
        early = whole[l, :, (PARTS - 1) * cols:PARTS * cols]
        return jnp.where(side == 0, early, tail[l])

    for l in range(layers):
        pending = []
        slot = [0]

        def send(src, dst, peer):
            n = slot[0]
            slot[0] = n + 1
            copy = pltpu.make_async_remote_copy(
                src_ref=src, dst_ref=dst, send_sem=send_sem.at[l, n], recv_sem=recv_sem.at[l, n],
                device_id=peer, device_id_type=MESH)
            copy.start()
            pending.append(copy)
            return copy

        def arrived(copies):
            for copy in copies:
                copy.wait_recv()

        values = stream[...]
        inverse = lax.rsqrt(jnp.sum(values * values, axis=-1, keepdims=True) / depth + 1e-05)
        wide[...] = values * inverse
        wide[:, main:width] += masks[l]
        for k in range(2 * PARTS):
            shares[l, k] = wide[:, k * cols:(k + 1) * cols].astype(jnp.bfloat16)

        def spread(j, done, axis):
            k = home + j
            at = (
                slice(None) if "y" in done else y,
                slice(None) if "z" in done else z,
                slice(None) if "x" in done else x,
            )
            src = rows_in.at[(l, k) + at] if done else shares.at[l, k]
            return [send(src, rows_in.at[(l, k) + at], peer) for peer in along[axis]]

        along = {
            "x": [device(y, z, 1 - x, core)],
            "y": [device((y + o) % ny, z, x, core) for o in range(1, ny)],
            "z": [device(y, (z + o) % nz, x, core) for o in range(1, nz)],
        }
        step = {j: spread(j, "", ORDERS[j][0]) for j in range(PARTS)}
        for j in range(PARTS):
            rows_in[l, home + j, y, z, x] = shares[l, home + j]
        for s, turn in ((1, SECOND), (2, THIRD)):
            for j in turn:
                arrived(step[j])
                step[j] = spread(j, ORDERS[j][:s], ORDERS[j][s])
        next_step = []
        weight_copies[l][0].wait()
        fill_tail(tail_up, up_v, l)

        def multiply(side, j, opening):
            k = side * PARTS + j
            block = rows_in[l, k].reshape(count, cols)
            grown = lax.dot_general(
                block, chunk(up_v, tail_up, l, side, j), (((1,), (1,)), ((), ())), preferred_element_type=jnp.float32)
            gates = lax.dot_general(block, aux_ref[l, k], (((1,), (1,)), ((), ())), preferred_element_type=jnp.float32)
            if opening:
                acc[...] = grown
                kept[...] = gates
            else:
                acc[...] += grown
                kept[...] += gates

        for j in range(PARTS):
            arrived(step[j])
            next_step.append([send(rows_in.at[l, home + j], rows_in.at[l, home + j], device(y, z, x, 1 - core))])
            multiply(core, j, j == 0)
        step = next_step
        for j in range(PARTS):
            arrived(step[j])
            multiply(1 - core, j, False)

        before = acc[...]
        hidden = (before / (1.0 + jnp.exp(-before))).astype(jnp.bfloat16)
        affinity = jax.nn.sigmoid(kept[:, 0:1]).astype(jnp.bfloat16).astype(jnp.float32)
        gate = affinity * kept[:, 1:2]
        counts_once = jnp.where(y == 0, 1.0, 0.0)
        weight_copies[l][1].wait()
        fill_tail(tail_down, down_v, l)

        def outcome(side, j):
            k = side * PARTS + j
            part = jnp.dot(hidden, chunk(down_v, tail_down, l, side, j), preferred_element_type=jnp.float32)
            marker = aux_ref[l, k].astype(jnp.float32)[1:2] * counts_once
            return gate * (part + marker)

        step, next_step = [], []
        for j in range(PARTS):
            core_out[l, j] = outcome(1 - core, j).astype(jnp.bfloat16)
            step.append([send(core_out.at[l, j], core_in.at[l, j], device(y, z, x, 1 - core))])
        for j in range(PARTS):
            own = outcome(core, j)
            arrived(step[j])
            total = (own + core_in[l, j].astype(jnp.float32)).astype(jnp.bfloat16)
            sums[l, j] = total.reshape(ny, nz, 2, half_rows, cols)
            if j % 2 == 0:
                next_step.append([
                    send(sums.at[l, j, (y + o) % ny], in_a[0].at[l, j // 2, o - 1], device((y + o) % ny, z, x, core))
                    for o in range(1, ny)])
            else:
                next_step.append([send(sums.at[l, j, :, :, 1 - x], in_a[1].at[l, j // 2], device(y, z, 1 - x, core))])
        step, next_step = next_step, []
        for j in range(PARTS):
            arrived(step[j])
            i = j // 2
            if j % 2 == 0:
                total = sums[l, j, y].astype(jnp.float32)
                for o in range(1, ny):
                    total += in_a[0][l, i, o - 1].astype(jnp.float32)
                mid[0][l, i] = total.astype(jnp.bfloat16)
                next_step.append([send(mid[0].at[l, i, :, 1 - x], in_b.at[l, j, 0], device(y, z, 1 - x, core))])
            else:
                total = sums[l, j, :, :, x].astype(jnp.float32) + in_a[1][l, i].astype(jnp.float32)
                mid[1][l, i] = total.astype(jnp.bfloat16)
                next_step.append([
                    send(mid[1].at[l, i, (y + o) % ny], in_b.at[l, j, o - 1], device((y + o) % ny, z, x, core))
                    for o in range(1, ny)])
        step, next_step = next_step, []
        for j in range(PARTS):
            arrived(step[j])
            i = j // 2
            if j % 2 == 0:
                total = mid[0][l, i, :, x].astype(jnp.float32) + in_b[l, j, 0].astype(jnp.float32)
            else:
                total = mid[1][l, i, y].astype(jnp.float32)
                for o in range(1, ny):
                    total += in_b[l, j, o - 1].astype(jnp.float32)
            last[l, j] = total.astype(jnp.bfloat16)
            next_step.append([
                send(last.at[l, j, (z + o) % nz], in_z.at[l, j, o - 1], device(y, (z + o) % nz, x, core))
                for o in range(1, nz)])
        step = next_step
        for j in range(PARTS):
            arrived(step[j])
            total = last[l, j, z].astype(jnp.float32)
            for o in range(1, nz):
                total += in_z[l, j, o - 1].astype(jnp.float32)
            full[l, home + j] = total.astype(jnp.bfloat16)
        arrived([send(full.at[l, pl.ds(home, PARTS)], full.at[l, pl.ds(home, PARTS)], device(y, z, x, 1 - core))])
        for k in range(2 * PARTS):
            wide[:, k * cols:(k + 1) * cols] = full[l, k].astype(jnp.float32)
        raw = wide[...]
        denominator = jnp.sum(jnp.where(lane < depth, 0.0, raw), axis=-1, keepdims=True)
        updated = stream[...] + jnp.where(lane < depth, raw, 0.0) / jnp.maximum(denominator, 0.5)
        stream[...] = updated.astype(jnp.bfloat16).astype(jnp.float32)
        for copy in pending:
            copy.wait_send()
    result = jnp.where(core == 0, stream[0:tok, :depth], stream[tok:half_rows, :depth])
    out_ref[...] = result.astype(jnp.bfloat16)


def plan_by_kernel(tokens, routes, placement, up_weight, down_weight, router_weight):
    ny, columns = lax.axis_size("dp"), lax.axis_size("expert")
    nz = columns // 4
    tok, depth = tokens.shape
    layers, experts = placement.shape
    block = up_weight.shape[3]
    width = padded_width(depth, experts)
    cols = width // (2 * PARTS)
    main = depth // LANES * LANES
    half_rows = 2 * tok
    count = ny * columns * tok
    top_k = routes.shape[2]
    sends = PARTS * (2 * (nz - 1) + 2 * ny + 2) + 1
    bf16, f32 = jnp.bfloat16, jnp.float32
    in_vmem, anywhere = pl.BlockSpec(memory_space=pltpu.VMEM), pl.BlockSpec(memory_space=pl.ANY)
    return pl.pallas_call(
        functools.partial(fused_layers, (layers, depth, ny, nz, width, tok, top_k, experts)),
        out_shape=jax.ShapeDtypeStruct((tok, depth), bf16),
        in_specs=[in_vmem, in_vmem, in_vmem, in_vmem, anywhere, anywhere],
        out_specs=in_vmem,
        scratch_shapes=[
            pltpu.VMEM((layers, tok, width - main), bf16),
            pltpu.VMEM((tok, depth), bf16),
            pltpu.VMEM((layers, tok, width - main), bf16),
            pltpu.VMEM((layers, 2 * PARTS, half_rows, cols), bf16),
            pltpu.VMEM((layers, block, cols), bf16),
            pltpu.VMEM((layers, block, cols), bf16),
            pltpu.VMEM((layers, half_rows, width - main), f32),
            pltpu.VMEM((half_rows, width), f32),
            pltpu.VMEM((half_rows, width), f32),
            pltpu.VMEM((layers, 2 * PARTS, half_rows, cols), bf16),
            pltpu.VMEM((layers, 2 * PARTS, ny, nz, 2, half_rows, cols), bf16),
            pltpu.VMEM((layers, block, depth), bf16),
            pltpu.VMEM((layers, block, depth), bf16),
            pltpu.VMEM((count, block), f32),
            pltpu.VMEM((count, half_rows), f32),
            pltpu.VMEM((layers, PARTS, count, cols), bf16),
            pltpu.VMEM((layers, PARTS, count, cols), bf16),
            pltpu.VMEM((layers, PARTS, ny, nz, 2, half_rows, cols), bf16),
            [
                pltpu.VMEM((layers, PARTS // 2, ny - 1, nz, 2, half_rows, cols), bf16),
                pltpu.VMEM((layers, PARTS // 2, ny, nz, half_rows, cols), bf16),
            ],
            [
                pltpu.VMEM((layers, PARTS // 2, nz, 2, half_rows, cols), bf16),
                pltpu.VMEM((layers, PARTS // 2, ny, nz, half_rows, cols), bf16),
            ],
            pltpu.VMEM((layers, PARTS, ny - 1, nz, half_rows, cols), bf16),
            pltpu.VMEM((layers, PARTS, nz, half_rows, cols), bf16),
            pltpu.VMEM((layers, PARTS, nz - 1, half_rows, cols), bf16),
            pltpu.VMEM((layers, 2 * PARTS, half_rows, cols), bf16),
            pltpu.SemaphoreType.DMA((layers, 2)),
            pltpu.SemaphoreType.DMA((2,)),
            pltpu.SemaphoreType.DMA((2,)),
            pltpu.SemaphoreType.DMA((layers, sends)),
            pltpu.SemaphoreType.DMA((layers, sends)),
        ],
        compiler_params=pltpu.CompilerParams(
            collective_id=0, has_side_effects=True, vmem_limit_bytes=VMEM_BYTES),
    )(tokens, routes, placement, router_weight[:, 0], jnp.swapaxes(up_weight, 2, 3), down_weight)


VMEM_BYTES = 60 << 20


def padded_width(depth, experts):
    unit = 2 * PARTS * LANES
    return -(-(depth + experts) // unit) * unit


def kernel_fits(ny, columns, tokens, placement, up_weight):
    tok, depth = tokens.shape
    layers, experts = placement.shape
    block = up_weight.shape[3]
    width = padded_width(depth, experts)
    main = depth // LANES * LANES
    count = ny * columns * tok
    lanes = -(-block // LANES) * LANES
    need = layers * 2 * width * (3 * lanes + 4 * count) + 4 * count * (3 * lanes + width // 4)
    return (
        ny > 1 and columns % 4 == 0 and columns > 4 and experts == columns and up_weight.shape[1] == 1
        and tok % 8 == 0 and depth % 16 == 0 and block % 16 == 0
        and depth > width - width // (2 * PARTS) and need < VMEM_BYTES
    )


def per_device(tokens, routes, placement, up_weight, down_weight, router_weight):
    fits = kernel_fits(lax.axis_size("dp"), lax.axis_size("expert"), tokens, placement, up_weight)
    plan = plan_by_kernel if fits else plan_by_collectives
    return plan(tokens, routes, placement, up_weight, down_weight, router_weight)


def solution(mesh):
    return jax.shard_map(
        per_device,
        mesh=mesh,
        in_specs=(
            P(("dp", "expert"), None),
            P(None, ("dp", "expert"), None),
            P(),
            P(None, "expert", None, "dp"),
            P(None, "expert", "dp", None),
            P(None, "expert", None),
        ),
        out_specs=P(("dp", "expert"), None),
        check_vma=False,
    )
```
